256 devices in a mesh: row: 32 (over y, x, core), col: 8 (over z).
Axes of the slice: x: 4, y: 4, z: 8, core: 2. Of those that a mesh axis runs over, the one named last changes fastest.
Arguments:
- features: bfloat16 [131072, 256], P(('row', 'col')), may hold values from -1 to 3
- in_degree: int32 [131072], P(('row', 'col')), may hold values from 512 to 2047
- tile_index: int32 [65536, 2], P(('row', 'col')), may hold values from 0 to 127, as said below
- tile_count: int32 [256], P(('row', 'col')), may hold values from 1 to 256, as said below
- adjacency_tiles: bfloat16 [65536, 128, 128], P(('row', 'col')), may hold values from 0 to 1, as said below
- projection: bfloat16 [512, 256], replicated, may hold values from -0.25 to 0.25
- out_bias: float32 [256], replicated, may hold values from -3 to 3
Outputs:
- hidden_out: bfloat16 [131072, 256], P(('row', 'col'))
The draws below stay inside these ranges and needn't reach their ends.
Inputs may be any that keep to these rules, and one draw needn't show every extreme that they name: `tile_index`: column 0 is a local row block below 32, column 1 a local column block below 128, in every slot. `tile_count`: slots at or beyond the count hold tiles and indices that must be ignored; some device has all 256 slots live in every draw. `adjacency_tiles`: entries are 0 or 1.
All inputs are finite; a program needn't handle non-finite values.
Results may differ from the reference program's by a relative error of at most 0.0034.
Values may be sent and summed in bfloat16 or wider, within the bound.
No kernel may reach another device: no remote copies, remote signals or barrier semaphores. Data moves between devices by JAX's collectives and lax.ppermute only.
A program may use at most 128 MiB of HBM per device.

```python
import jax
import jax.numpy as jnp
from jax import lax

F = 256
H = 256
TILE = 128
VB_DEV = 4
MAX_TILES = 256
RB = 32
CB = 128
V = 131072
N_ROW = 32
N_COL = 8


def draw_tile_index(key, part):
    slots = N_ROW * N_COL * MAX_TILES
    row_part = jax.random.randint(jax.random.fold_in(key, 11), (slots,), 0, VB_DEV * N_COL)
    col_part = jax.random.randint(jax.random.fold_in(key, 12), (slots,), 0, VB_DEV * N_ROW)
    return jnp.stack([row_part, col_part], axis=1).astype(jnp.int32)


def draw_tile_count(key, part):
    devices = N_ROW * N_COL
    counts = jax.random.randint(jax.random.fold_in(key, 21), (devices,), max(1, MAX_TILES // 8), MAX_TILES + 1)
    fullest = jax.random.randint(jax.random.fold_in(key, 22), (), 0, devices)
    placed = jnp.arange(devices, dtype=jnp.int32) == fullest
    return jnp.where(placed, MAX_TILES, counts).astype(jnp.int32)


def draw_adjacency_tiles(key, part):
    shape = (N_ROW * N_COL * MAX_TILES, TILE, TILE)
    uniform_draw = jax.random.uniform(jax.random.fold_in(key, 31), shape, jnp.float32)
    return jnp.where(uniform_draw < 0.25, 1.0, 0.0).astype(jnp.float32).astype(jnp.bfloat16)


def place_ends(drawn, own_key, low, largest):
    longest = drawn.shape.index(max(drawn.shape))
    spots = []
    for shift in (0, 1):
        where = [jax.random.randint(jax.random.fold_in(own_key, axis), (), 0, length) for axis, length in enumerate(drawn.shape)]
        where[longest] = (where[longest] + shift) % drawn.shape[longest]
        spots.append(tuple(where))
    return drawn.at[spots[0]].set(low).at[spots[1]].set(largest)


def shard_levels(own_key, extent, split, low, largest):
    def one(axis_at, parts):
        heights = jax.random.uniform(jax.random.fold_in(jax.random.fold_in(own_key, 6), axis_at), (parts,), jnp.float32, low / len(split), largest / len(split))
        return jnp.repeat(jnp.exp(heights), extent[axis_at] // parts).reshape((-1,) + (1,) * (len(extent) - axis_at - 1))

    level = one(*split[0])
    for cut in split[1:]:
        level = level * one(*cut)
    return level


def centred(key, dims, width, limit, held_as=jnp.bfloat16):
    array = jax.random.normal(key, dims, jnp.float32) * width
    return jnp.minimum(jnp.maximum(array, -limit), limit).astype(held_as)


def setup_inputs(seed: int = 0) -> dict:
    keys = jax.random.split(jax.random.key(seed), 8)
    features = jnp.clip(-1.0 + 4.0 * jax.random.uniform(keys[0], (V, F), jnp.float32) ** shard_levels(keys[0], (V, F), ((0, 256),), -0.2, 0.2), -1.0, 3.0).astype(jnp.bfloat16)
    in_degree = place_ends(jax.random.randint(keys[1], (V,), max(1, MAX_TILES * TILE // (VB_DEV * 16)), max(2, MAX_TILES * TILE // (VB_DEV * 4))), jax.random.fold_in(keys[1], 1), max(1, MAX_TILES * TILE // (VB_DEV * 16)), (max(2, MAX_TILES * TILE // (VB_DEV * 4))) - 1).astype(jnp.int32)
    tile_index = draw_tile_index(jax.random.fold_in(keys[7], 71), 0)
    tile_count = draw_tile_count(jax.random.fold_in(keys[7], 71), 0)
    adjacency_tiles = draw_adjacency_tiles(jax.random.fold_in(keys[7], 71), 0)
    projection = centred(keys[5], (2 * F, H), (2 * F) ** -0.5, 0.25)
    out_bias = centred(keys[6], (H,), 0.5, 3.0, jnp.float32)
    return {"features": features, "in_degree": in_degree, "tile_index": tile_index, "tile_count": tile_count, "adjacency_tiles": adjacency_tiles, "projection": projection, "out_bias": out_bias}


def device_partial(column_rows, slot_index, live_count, slot_tiles):
    blocks = column_rows.reshape(CB, TILE, F).astype(jnp.float32)[slot_index[:, 1]]
    alive = (jnp.arange(MAX_TILES, dtype=jnp.int32) < live_count).astype(jnp.float32)
    masked = slot_tiles.astype(jnp.float32) * alive[:, None, None]
    product = jnp.einsum("kij,kjf->kif", masked, blocks)
    summed = jax.ops.segment_sum(product, slot_index[:, 0], num_segments=RB)
    return summed.reshape(RB * TILE, F)


def reference(features, in_degree, tile_index, tile_count, adjacency_tiles, projection, out_bias):
    span = VB_DEV * TILE
    grouped = features.reshape(N_ROW, N_COL, span, F)

    def per_row(row_id):
        def per_col(running, col_id):
            column_rows = jnp.take(grouped, col_id, axis=1).reshape(N_ROW * span, F)
            device = row_id * N_COL + col_id
            slot_index = lax.dynamic_slice_in_dim(tile_index, device * MAX_TILES, MAX_TILES, 0)
            slot_tiles = lax.dynamic_slice_in_dim(adjacency_tiles, device * MAX_TILES, MAX_TILES, 0)
            live_count = tile_count[device]
            return running + device_partial(column_rows, slot_index, live_count, slot_tiles), None

        zeroed = jnp.zeros((RB * TILE, F), jnp.float32)
        summed, _ = lax.scan(per_col, zeroed, jnp.arange(N_COL, dtype=jnp.int32))
        return summed

    sums = lax.map(per_row, jnp.arange(N_ROW, dtype=jnp.int32)).reshape(V, F)
    neighbour_mean = (sums / in_degree[:, None].astype(jnp.float32)).astype(jnp.bfloat16)
    joined = jnp.concatenate([features, neighbour_mean], axis=1)
    mixed = jnp.dot(joined, projection, preferred_element_type=jnp.float32) + out_bias[None, :]
    return jnp.maximum(mixed, 0.0).astype(jnp.bfloat16)
```

```python
import jax
import jax.numpy as jnp
from jax import lax
from jax.experimental import pallas as pl
from jax.experimental.pallas import tpu as pltpu
from jax.sharding import PartitionSpec as P


NY, NX, NC, NZ = 4, 4, 2, 8
TILE = 128
CHUNK = 32
UNROLL = 8


def row_perm(source_of):
    pairs = []
    for y in range(NY):
        for x in range(NX):
            for c in range(NC):
                sy, sx, sc = source_of(y, x, c)
                src = ((sy % NY) * NX + sx % NX) * NC + sc % NC
                pairs.append((src, (y * NX + x) * NC + c))
    return pairs


def first_phase(d):
    return row_perm(lambda y, x, c: (y, x + d, c) if c == 0 else (y + d, x, c))


def second_phase(d):
    return row_perm(lambda y, x, c: (y + d, x, c) if c == 0 else (y, x + d, c))


CORE_SWAP = row_perm(lambda y, x, c: (y, x, c + 1))


def gather_features(features):
    near = [features] + [lax.ppermute(features, "row", first_phase(d)) for d in (1, 2, 3)]
    near = jnp.concatenate(near, axis=0)
    own = [near] + [lax.ppermute(near, "row", second_phase(d)) for d in (1, 2, 3)]
    other = [lax.ppermute(piece, "row", CORE_SWAP) for piece in own]
    return own, other


def slot_tables(tile_index):
    row_id = lax.axis_index("row")
    col_id = lax.axis_index("col")
    y, x, core = row_id // (NX * NC), (row_id // NC) % NX, row_id % NC
    rows, cols = tile_index[:, 0], tile_index[:, 1]
    owner, sub = cols // 4, cols % 4
    dy = (owner // (NX * NC) - y) % NY
    dx = (owner // NC - x) % NX
    oc = owner % NC
    inner = jnp.where(oc == 0, dy * 4 + dx, dx * 4 + dy)
    half = (oc + core) % 2
    slot_col = (half * 16 + inner) * 4 + sub
    slot_row = ((rows // 4 - col_id) % NZ) * 4 + rows % 4
    return slot_row * TILE, slot_col * TILE


def block_kernel(count_ref, row_ref, col_ref, tiles_hbm, *rest):
    pieces, (out_ref, table, tiles, sems) = rest[:-4], rest[-4:]
    n_chunks = tiles_hbm.shape[0] // CHUNK
    for g in range(n_chunks):
        pltpu.make_async_copy(tiles_hbm.at[pl.ds(g * CHUNK, CHUNK)], tiles.at[pl.ds(g * CHUNK, CHUNK)], sems.at[g]).start()
    out_ref[...] = jnp.zeros_like(out_ref)
    span = pieces[0].shape[0]
    for i, piece in enumerate(pieces):
        table[pl.ds(i * span, span), :] = piece[...]
    count = count_ref[0]
    for g in range(n_chunks):
        pltpu.make_async_copy(tiles_hbm.at[pl.ds(g * CHUNK, CHUNK)], tiles.at[pl.ds(g * CHUNK, CHUNK)], sems.at[g]).wait()
        turns = jnp.clip((count - g * CHUNK + UNROLL - 1) // UNROLL, 0, CHUNK // UNROLL)

        @pl.loop(0, turns)
        def _(t):
            for u in range(UNROLL):
                k = g * CHUNK + t * UNROLL + u
                r = pl.multiple_of(row_ref[k], TILE)
                c = pl.multiple_of(col_ref[k], TILE)
                tile = jnp.where(k < count, tiles[k], jnp.zeros((TILE, TILE), jnp.bfloat16))
                term = jnp.dot(tile, table[pl.ds(c, TILE), :], preferred_element_type=jnp.float32)
                out_ref[pl.ds(r, TILE), :] += term


def block_sums(count, rows, cols, tiles, pieces, n_rows):
    width = pieces[0].shape[1]
    smem = pl.BlockSpec(memory_space=pltpu.SMEM)
    vmem = pl.BlockSpec(memory_space=pltpu.VMEM)
    return pl.pallas_call(
        block_kernel,
        out_shape=jax.ShapeDtypeStruct((n_rows, width), jnp.float32),
        in_specs=[smem, smem, smem, pl.BlockSpec(memory_space=pl.ANY)] + [vmem] * len(pieces),
        out_specs=vmem,
        scratch_shapes=[
            pltpu.VMEM((sum(p.shape[0] for p in pieces), width), jnp.bfloat16),
            pltpu.VMEM(tiles.shape, jnp.bfloat16),
            pltpu.SemaphoreType.DMA((tiles.shape[0] // CHUNK,)),
        ],
        compiler_params=pltpu.CompilerParams(vmem_limit_bytes=40 * 1024 * 1024),
        name="block_sums",
    )(count, rows, cols, tiles, *pieces)


UP = [(i, (i + 1) % NZ) for i in range(NZ)]
DOWN = [(i, (i - 1) % NZ) for i in range(NZ)]


def reduce_over_col(partial_value):
    parts = partial_value.reshape(NZ, -1, partial_value.shape[1])
    span = parts.shape[1]
    half = span // 2

    def narrow(v):
        return v.astype(jnp.bfloat16)

    def wide(v):
        return v.astype(jnp.float32)

    up = lax.ppermute(narrow(parts[4, :half]), "col", UP)
    down = lax.ppermute(narrow(parts[4, half:]), "col", DOWN)
    up = jnp.concatenate([wide(up) + parts[3, :half], parts[3, half:]], axis=0)
    down = jnp.concatenate([parts[5, :half], wide(down) + parts[5, half:]], axis=0)
    for k in (2, 1):
        up = wide(lax.ppermute(narrow(up), "col", UP)) + parts[k]
        down = wide(lax.ppermute(narrow(down), "col", DOWN)) + parts[8 - k]
    up = lax.ppermute(narrow(up), "col", UP)
    down = lax.ppermute(narrow(down), "col", DOWN)
    return parts[0] + wide(up) + wide(down)


def local(features, in_degree, tile_index, tile_count, adjacency_tiles, projection, out_bias):
    feat_width = features.shape[1]
    rows, cols = slot_tables(tile_index)
    own, other = gather_features(features)
    n_rows = features.shape[0] * NZ
    partial_value = block_sums(tile_count, rows, cols, adjacency_tiles, own + other, n_rows)
    own_sums = reduce_over_col(partial_value)
    neighbour_mean = (own_sums / in_degree[:, None].astype(jnp.float32)).astype(jnp.bfloat16)
    mixed = jnp.dot(features, projection[:feat_width], preferred_element_type=jnp.float32)
    mixed = mixed + jnp.dot(neighbour_mean, projection[feat_width:], preferred_element_type=jnp.float32)
    return jnp.maximum(mixed + out_bias[None, :], 0.0).astype(jnp.bfloat16)


def solution(mesh):
    return jax.shard_map(
        local,
        mesh=mesh,
        in_specs=(
            P(("row", "col"), None),
            P(("row", "col")),
            P(("row", "col"), None),
            P(("row", "col")),
            P(("row", "col"), None, None),
            P(),
            P(),
        ),
        out_specs=P(("row", "col"), None),
        check_vma=False,
    )
```

```python
import jax
import jax.numpy as jnp
from jax import lax
from jax.experimental import pallas as pl
from jax.experimental.pallas import tpu as pltpu
from jax.sharding import PartitionSpec as P


NY, NX, NC, NZ = 4, 4, 2, 8
TILE = 128
UNROLL = 8
PAIRS = 160
GROUP_STARTS = (0, 4, 12, 20, 28, 32)


def device_at(y, x, c):
    return ((y % NY) * NX + x % NX) * NC + c % NC


def row_perm(source_of):
    return [
        (device_at(*source_of(y, x, c)), device_at(y, x, c))
        for y in range(NY)
        for x in range(NX)
        for c in range(NC)
    ]


NEAR_GROUPS = [[device_at(y, x, 0) for x in range(NX)] for y in range(NY)]
NEAR_GROUPS += [[device_at(y, x, 1) for y in range(NY)] for x in range(NX)]


def far_perm(d):
    return row_perm(lambda y, x, c: (y + d, x, c) if c == 0 else (y, x + d, c))


CORE_SWAP = row_perm(lambda y, x, c: (y, x, c + 1))


def gather_features(features):
    span, width = features.shape
    copies = jnp.broadcast_to(features[None], (NX, span, width))
    near = lax.all_to_all(copies, "row", 0, 0, axis_index_groups=NEAR_GROUPS, tiled=True).reshape(NX * span, width)
    first, second = near[: 2 * span], near[2 * span :]
    back, ahead = far_perm(-1), far_perm(1)
    back_first = lax.ppermute(first, "row", back)
    ahead_second = lax.ppermute(second, "row", ahead)
    back_second = lax.ppermute(second, "row", back)
    ahead_first = lax.ppermute(first, "row", ahead)
    far_first = lax.ppermute(back_first, "row", back)
    far_second = lax.ppermute(ahead_second, "row", ahead)
    own = [near, ahead_first, ahead_second, far_first, far_second, back_first, back_second]
    other = [lax.ppermute(piece, "row", CORE_SWAP) for piece in own]
    return jnp.concatenate(own + other, axis=0)


def slot_plan(tile_index, count):
    slots = tile_index.shape[0]
    row_id = lax.axis_index("row")
    col_id = lax.axis_index("col")
    y, x, core = row_id >> 3, (row_id >> 1) & 3, row_id & 1
    rows, cols = tile_index[:, 0], tile_index[:, 1]
    owner, sub = cols >> 2, cols & 3
    oy, ox, oc = owner >> 3, (owner >> 1) & 3, owner & 1
    inner = jnp.where(oc == 0, ((oy - y) & 3) * 4 + ox, ((ox - x) & 3) * 4 + oy)
    slot_col = ((oc ^ core) * 16 + inner) * 4 + sub
    chunk = ((rows >> 2) - col_id) & 7
    turn = jnp.where(chunk == 0, 7, jnp.where(chunk < 4, 7 - 2 * chunk, 2 * chunk - 8))
    live = jnp.arange(slots, dtype=jnp.int32) < count
    key = jnp.where(live, turn * 4 + (rows & 3), 64)

    def total(mask, value, axis):
        return jnp.sum(jnp.where(mask, value, 0), axis=axis, dtype=jnp.int32)

    ids = jnp.arange(slots, dtype=jnp.int32)
    blocks = jnp.arange(NZ * 4, dtype=jnp.int32)
    place = total((key[:, None] == key[None, :]) & (ids[None, :] < ids[:, None]), 1, 1)
    held = total(key[None, :] == blocks[:, None], 1, 1)
    pairs = (held + 1) >> 1
    ahead = total(blocks[None, :] < key[:, None], pairs[None, :], 1)
    spot = jnp.where(live, 2 * ahead + place, -1)
    bounds = total(blocks[None, :] < jnp.array(GROUP_STARTS, jnp.int32)[:, None], pairs[None, :], 1)
    slot_ids = jnp.arange(2 * PAIRS, dtype=jnp.int32)
    hit = spot[None, :] == slot_ids[:, None]
    tile_of = total(hit, ids[None, :] + 1, 1) - 1
    col_of = total(hit, slot_col[None, :], 1) * TILE
    row_of = total(spot[None, :] == 2 * slot_ids[:PAIRS, None], key[None, :], 1) * TILE
    return jnp.concatenate([tile_of, col_of, row_of, bounds])


def block_kernel(group, plan, tiles, table, out_ref):
    base = GROUP_STARTS[group] * TILE
    start, stop = plan[5 * PAIRS + group], plan[5 * PAIRS + group + 1]
    out_ref[...] = jnp.zeros_like(out_ref)

    @pl.loop(0, (stop - start + UNROLL - 1) // UNROLL)
    def _(t):
        for u in range(UNROLL):
            pair = start + t * UNROLL + u
            live = pair < stop
            pair = jnp.minimum(pair, PAIRS - 1)
            lhs, rhs = [], []
            for side in range(2):
                k = plan[2 * pair + side]
                tile = tiles[jnp.maximum(k, 0)]
                lhs.append(jnp.where(live & (k >= 0), tile, jnp.zeros_like(tile)))
                c = pl.multiple_of(plan[2 * PAIRS + 2 * pair + side], TILE)
                rhs.append(table[pl.ds(c, TILE), :])
            term = jnp.dot(jnp.concatenate(lhs, 1), jnp.concatenate(rhs, 0), preferred_element_type=jnp.float32)
            r = pl.multiple_of(jnp.where(live, plan[4 * PAIRS + pair] - base, 0), TILE)
            out_ref[pl.ds(r, TILE), :] += term


def block_sums(group, plan, tiles, table):
    blocks = GROUP_STARTS[group + 1] - GROUP_STARTS[group]
    width = table.shape[1]
    vmem = pl.BlockSpec(memory_space=pltpu.VMEM)
    return pl.pallas_call(
        lambda *refs: block_kernel(group, *refs),
        out_shape=jax.ShapeDtypeStruct((blocks * TILE, width), jnp.float32),
        in_specs=[pl.BlockSpec(memory_space=pltpu.SMEM), vmem, vmem],
        out_specs=vmem,
        compiler_params=pltpu.CompilerParams(vmem_limit_bytes=32 * 1024 * 1024),
        cost_estimate=pl.CostEstimate(flops=blocks * 100_000_000, bytes_accessed=blocks * 500_000, transcendentals=0),
        name=f"block_sums_{group}",
    )(plan, tiles, table)


UP = [(i, (i + 1) % NZ) for i in range(NZ)]
DOWN = [(i, (i - 1) % NZ) for i in range(NZ)]


def narrow(v):
    return v.astype(jnp.bfloat16)


def wide(v):
    return v.astype(jnp.float32)


def sums_over_col(plan, tiles, table):
    part = block_sums(0, plan, tiles, table)
    span = part.shape[0]
    half = span // 2
    up = lax.ppermute(narrow(part[:half]), "col", UP)
    down = lax.ppermute(narrow(part[half:]), "col", DOWN)
    part = block_sums(1, plan, tiles, table)
    up = jnp.concatenate([wide(up) + part[:half], part[half:span]], axis=0)
    down = jnp.concatenate([part[span : span + half], wide(down) + part[span + half :]], axis=0)
    for group in (2, 3):
        up = lax.ppermute(narrow(up), "col", UP)
        down = lax.ppermute(narrow(down), "col", DOWN)
        part = block_sums(group, plan, tiles, table)
        up = wide(up) + part[:span]
        down = wide(down) + part[span:]
    up = lax.ppermute(narrow(up), "col", UP)
    down = lax.ppermute(narrow(down), "col", DOWN)
    part = block_sums(4, plan, tiles, table)
    return part + wide(up) + wide(down)


def local(features, in_degree, tile_index, tile_count, adjacency_tiles, projection, out_bias):
    feat_width = features.shape[1]
    plan = slot_plan(tile_index, tile_count[0])
    table = gather_features(features)
    own_sums = sums_over_col(plan, adjacency_tiles, table)
    neighbour_mean = (own_sums / in_degree[:, None].astype(jnp.float32)).astype(jnp.bfloat16)
    mixed = jnp.dot(features, projection[:feat_width], preferred_element_type=jnp.float32)
    mixed = mixed + jnp.dot(neighbour_mean, projection[feat_width:], preferred_element_type=jnp.float32)
    return jnp.maximum(mixed + out_bias[None, :], 0.0).astype(jnp.bfloat16)


def solution(mesh):
    return jax.shard_map(
        local,
        mesh=mesh,
        in_specs=(
            P(("row", "col"), None),
            P(("row", "col")),
            P(("row", "col"), None),
            P(("row", "col")),
            P(("row", "col"), None, None),
            P(),
            P(),
        ),
        out_specs=P(("row", "col"), None),
        check_vma=False,
    )
```

```python
import jax
import jax.numpy as jnp
from jax import lax
from jax.experimental import pallas as pl
from jax.experimental.pallas import tpu as pltpu
from jax.sharding import PartitionSpec as P


NY, NX, NC, NZ = 4, 4, 2, 8
TILE = 128
UNROLL = 8
PAIRS = 160
GROUP_STARTS = (0, 4, 12, 20, 28, 32)


def device_at(y, x, c):
    return ((y % NY) * NX + x % NX) * NC + c % NC


def row_perm(source_of):
    return [
        (device_at(*source_of(y, x, c)), device_at(y, x, c))
        for y in range(NY)
        for x in range(NX)
        for c in range(NC)
    ]


def near_perm(d):
    return row_perm(lambda y, x, c: (y, x + d, c) if c == 0 else (y + d, x, c))


def far_perm(d):
    return row_perm(lambda y, x, c: (y + d, x, c) if c == 0 else (y, x + d, c))


CORE_SWAP = row_perm(lambda y, x, c: (y, x, c + 1))


def gather_features(features):
    near = {d: lax.ppermute(features, "row", near_perm(d)) for d in (1, 3, 2)}
    first = jnp.concatenate([features, near[1]], axis=0)
    second = jnp.concatenate([near[3], near[2]], axis=0)
    back, ahead = far_perm(-1), far_perm(1)
    back_first = lax.ppermute(first, "row", back)
    ahead_first = lax.ppermute(first, "row", ahead)
    ahead_second = lax.ppermute(second, "row", ahead)
    back_second = lax.ppermute(second, "row", back)
    far_first = lax.ppermute(back_first, "row", back)
    far_second = lax.ppermute(ahead_second, "row", ahead)
    own = [first, second, ahead_first, ahead_second, far_first, far_second, back_first, back_second]
    other = [lax.ppermute(piece, "row", CORE_SWAP) for piece in own]
    return jnp.concatenate(own + other, axis=0)


def slot_plan(tile_index, count):
    slots = tile_index.shape[0]
    row_id = lax.axis_index("row")
    col_id = lax.axis_index("col")
    y, x, core = row_id >> 3, (row_id >> 1) & 3, row_id & 1
    rows, cols = tile_index[:, 0], tile_index[:, 1]
    owner, sub = cols >> 2, cols & 3
    oy, ox, oc = owner >> 3, (owner >> 1) & 3, owner & 1
    dy, dx = (oy - y) & 3, (ox - x) & 3
    far, near = jnp.where(oc == 0, dy, dx), jnp.where(oc == 0, dx, dy)
    inner = far * 4 + (near ^ (near >> 1))
    slot_col = ((oc ^ core) * 16 + inner) * 4 + sub
    chunk = ((rows >> 2) - col_id) & 7
    turn = jnp.where(chunk == 0, 7, jnp.where(chunk < 4, 7 - 2 * chunk, 2 * chunk - 8))
    live = jnp.arange(slots, dtype=jnp.int32) < count
    key = jnp.where(live, turn * 4 + (rows & 3), 64)

    def total(mask, value, axis):
        return jnp.sum(jnp.where(mask, value, 0), axis=axis, dtype=jnp.int32)

    ids = jnp.arange(slots, dtype=jnp.int32)
    blocks = jnp.arange(NZ * 4, dtype=jnp.int32)
    place = total((key[:, None] == key[None, :]) & (ids[None, :] < ids[:, None]), 1, 1)
    held = total(key[None, :] == blocks[:, None], 1, 1)
    pairs = (held + 1) >> 1
    ahead = total(blocks[None, :] < key[:, None], pairs[None, :], 1)
    spot = jnp.where(live, 2 * ahead + place, -1)
    bounds = total(blocks[None, :] < jnp.array(GROUP_STARTS, jnp.int32)[:, None], pairs[None, :], 1)
    slot_ids = jnp.arange(2 * PAIRS, dtype=jnp.int32)
    hit = spot[None, :] == slot_ids[:, None]
    tile_of = total(hit, ids[None, :] + 1, 1) - 1
    col_of = total(hit, slot_col[None, :], 1) * TILE
    row_of = total(spot[None, :] == 2 * slot_ids[:PAIRS, None], key[None, :], 1) * TILE
    return jnp.concatenate([tile_of, col_of, row_of, bounds])


def block_kernel(group, plan, tiles, table, out_ref):
    base = GROUP_STARTS[group] * TILE
    start, stop = plan[5 * PAIRS + group], plan[5 * PAIRS + group + 1]
    out_ref[...] = jnp.zeros_like(out_ref)

    @pl.loop(0, (stop - start + UNROLL - 1) // UNROLL)
    def _(t):
        for u in range(UNROLL):
            pair = start + t * UNROLL + u
            live = pair < stop
            pair = jnp.minimum(pair, PAIRS - 1)
            lhs, rhs = [], []
            for side in range(2):
                k = plan[2 * pair + side]
                tile = tiles[jnp.maximum(k, 0)]
                lhs.append(jnp.where(live & (k >= 0), tile, jnp.zeros_like(tile)))
                c = pl.multiple_of(plan[2 * PAIRS + 2 * pair + side], TILE)
                rhs.append(table[pl.ds(c, TILE), :])
            term = jnp.dot(jnp.concatenate(lhs, 1), jnp.concatenate(rhs, 0), preferred_element_type=jnp.float32)
            r = pl.multiple_of(jnp.where(live, plan[4 * PAIRS + pair] - base, 0), TILE)
            out_ref[pl.ds(r, TILE), :] += term


def block_sums(group, plan, tiles, table):
    blocks = GROUP_STARTS[group + 1] - GROUP_STARTS[group]
    width = table.shape[1]
    vmem = pl.BlockSpec(memory_space=pltpu.VMEM)
    return pl.pallas_call(
        lambda *refs: block_kernel(group, *refs),
        out_shape=jax.ShapeDtypeStruct((blocks * TILE, width), jnp.float32),
        in_specs=[pl.BlockSpec(memory_space=pltpu.SMEM), vmem, vmem],
        out_specs=vmem,
        compiler_params=pltpu.CompilerParams(vmem_limit_bytes=32 * 1024 * 1024),
        cost_estimate=pl.CostEstimate(flops=blocks * 100_000_000, bytes_accessed=blocks * 500_000, transcendentals=0),
        name=f"block_sums_{group}",
    )(plan, tiles, table)


UP = [(i, (i + 1) % NZ) for i in range(NZ)]
DOWN = [(i, (i - 1) % NZ) for i in range(NZ)]


def narrow(v):
    return v.astype(jnp.bfloat16)


def wide(v):
    return v.astype(jnp.float32)


def after(values, earlier):
    return lax.optimization_barrier((tuple(values), tuple(earlier)))[0]


def send(name, up, down):
    with jax.named_scope(name):
        return lax.ppermute(up, "col", UP), lax.ppermute(down, "col", DOWN)


def sums_over_col(plan, tiles, table):
    def sums(group, earlier):
        held = after((plan,), earlier)[0] if earlier else plan
        with jax.named_scope(f"sums_{group}"):
            return block_sums(group, held, tiles, table)

    part = sums(0, ())
    span = part.shape[0]
    half = span // 2
    one = narrow(part[:half]), narrow(part[half:])
    one_in = send("one_0", *one)
    part = sums(1, one)
    two = narrow(part[half:span]), narrow(part[span : span + half])
    two_in = send("two_1", *two)
    for group in (1, 2, 3):
        if group > 1:
            two_in = after(two_in, one)
            two = narrow(wide(two_in[0]) + part[half:span]), narrow(wide(two_in[1]) + part[span : span + half])
            two_in = send(f"two_{group}", *two)
        one_in = after(one_in, two)
        one = narrow(wide(one_in[0]) + part[:half]), narrow(wide(one_in[1]) + part[span + half :])
        one_in = send(f"one_{group}", *one)
        part = sums(group + 1, two)
    upper = part[:half] + wide(one_in[0]) + wide(two_in[1])
    lower = part[half:] + wide(two_in[0]) + wide(one_in[1])
    return jnp.concatenate([upper, lower], axis=0)


def local(features, in_degree, tile_index, tile_count, adjacency_tiles, projection, out_bias):
    feat_width = features.shape[1]
    plan = slot_plan(tile_index, tile_count[0])
    table = gather_features(features)
    own_sums = sums_over_col(plan, adjacency_tiles, table)
    neighbour_mean = (own_sums / in_degree[:, None].astype(jnp.float32)).astype(jnp.bfloat16)
    mixed = jnp.dot(features, projection[:feat_width], preferred_element_type=jnp.float32)
    mixed = mixed + jnp.dot(neighbour_mean, projection[feat_width:], preferred_element_type=jnp.float32)
    return jnp.maximum(mixed + out_bias[None, :], 0.0).astype(jnp.bfloat16)


def solution(mesh):
    return jax.shard_map(
        local,
        mesh=mesh,
        in_specs=(
            P(("row", "col"), None),
            P(("row", "col")),
            P(("row", "col"), None),
            P(("row", "col")),
            P(("row", "col"), None, None),
            P(),
            P(),
        ),
        out_specs=P(("row", "col"), None),
        check_vma=False,
    )
```
